8 devices in a mesh: data: 4 (over z, y, x), stage: 2 (over core).
Axes of the slice: x: 2, y: 2, z: 1, core: 2. Of those that a mesh axis runs over, the one named last changes fastest.
Arguments:
- master_up: float32 [2, 896, 4864], P('stage', 'data')
- master_down: float32 [2, 4864, 896], P('stage', 'data')
- moment1_up: float32 [2, 896, 4864], P('stage', 'data')
- moment2_up: float32 [2, 896, 4864], P('stage', 'data')
- moment1_down: float32 [2, 4864, 896], P('stage', 'data')
- moment2_down: float32 [2, 4864, 896], P('stage', 'data')
- compute_up: bfloat16 [2, 896, 4864], P('stage')
- compute_down: bfloat16 [2, 4864, 896], P('stage')
- accum_up: float32 [4, 2, 896, 4864], P('data', 'stage')
- accum_down: float32 [4, 2, 4864, 896], P('data', 'stage')
- stage_acts: bfloat16 [2, 8192, 896], P('stage', 'data')
- loss_grad: bfloat16 [8192, 896], P('data')
- next_micro: bfloat16 [16, 8192, 896], P(None, 'data')
- learn_rate: float32 [], replicated
- max_norm: float32 [], replicated
Outputs:
- output 1: float32 [2, 896, 4864], P('stage', 'data')
- output 2: float32 [2, 4864, 896], P('stage', 'data')
- output 3: float32 [2, 896, 4864], P('stage', 'data')
- output 4: float32 [2, 896, 4864], P('stage', 'data')
- output 5: float32 [2, 4864, 896], P('stage', 'data')
- output 6: float32 [2, 4864, 896], P('stage', 'data')
- output 7: bfloat16 [16, 8192, 896], P(None, 'data')
All inputs are finite; a program needn't handle non-finite values.
Results may differ from the reference program's by a relative error of at most 0.00562341.
Values are sent between devices in bfloat16 or wider.
A program may use at most 1 GiB of HBM per device.

```python
import jax
import jax.numpy as jnp
from jax import lax

D_MODEL = 896
FF_WIDTH = 4864
STAGES = 2
REPLICAS = 4
TOKENS_DEV = 2048
MICRO_NEXT = 16
STEP_NUM = 10

BETA_ONE = 0.9
BETA_TWO = 0.95
ADAM_EPS = 1e-8
WEIGHT_DECAY = 0.1
NORM_EPS = 1e-6
BIAS_ONE = 1.0 - BETA_ONE ** STEP_NUM
BIAS_TWO = 1.0 - BETA_TWO ** STEP_NUM


def gelu_tanh(pre_act):
    return jax.nn.gelu(pre_act, approximate=True)


def stage_forward(stage_in, w_up, w_down):
    pre_act = jnp.dot(stage_in, w_up, preferred_element_type=jnp.float32)
    hidden = gelu_tanh(pre_act).astype(jnp.bfloat16)
    branch = jnp.dot(hidden, w_down, preferred_element_type=jnp.float32)
    return (stage_in.astype(jnp.float32) + branch).astype(jnp.bfloat16)


def stage_backward(stage_in, grad_in, w_up, w_down):
    pre_act = jnp.dot(stage_in, w_up, preferred_element_type=jnp.float32)
    hidden, gelu_pull = jax.vjp(gelu_tanh, pre_act)
    hidden = hidden.astype(jnp.bfloat16)
    dw_down = jnp.dot(hidden.T, grad_in, preferred_element_type=jnp.float32)
    d_hidden = jnp.dot(grad_in, w_down.T, preferred_element_type=jnp.float32)
    d_pre = gelu_pull(d_hidden)[0].astype(jnp.bfloat16)
    dw_up = jnp.dot(stage_in.T, d_pre, preferred_element_type=jnp.float32)
    d_in = grad_in.astype(jnp.float32) + jnp.dot(d_pre, w_up.T, preferred_element_type=jnp.float32)
    return dw_up, dw_down, d_in.astype(jnp.bfloat16)


def replica_grads(compute_up, compute_down, acts_one, grad_one):
    def stage_step(grad_in, stage_items):
        dw_up, dw_down, d_in = stage_backward(stage_items[2], grad_in, stage_items[0], stage_items[1])
        return d_in, (dw_up, dw_down)
    first_grad, stage_grads = lax.scan(stage_step, grad_one, (compute_up, compute_down, acts_one), reverse=True)
    return stage_grads


def batch_grads(compute_up, compute_down, stage_acts, loss_grad):
    acts_rep = stage_acts.reshape(STAGES, REPLICAS, TOKENS_DEV, D_MODEL).transpose(1, 0, 2, 3)
    grad_rep = loss_grad.reshape(REPLICAS, TOKENS_DEV, D_MODEL)
    zero_up = jnp.zeros((STAGES, D_MODEL, FF_WIDTH), jnp.float32)
    zero_down = jnp.zeros((STAGES, FF_WIDTH, D_MODEL), jnp.float32)
    zero_sq = jnp.zeros((STAGES,), jnp.float32)

    def replica_step(carry, items):
        sum_up, sum_down, sq_up, sq_down = carry
        dw_up, dw_down = replica_grads(compute_up, compute_down, items[0], items[1])
        carry_new = (sum_up + dw_up, sum_down + dw_down,
                     sq_up + jnp.sum(dw_up * dw_up, axis=(1, 2)),
                     sq_down + jnp.sum(dw_down * dw_down, axis=(1, 2)))
        return carry_new, None
    totals, unused = lax.scan(replica_step, (zero_up, zero_down, zero_sq, zero_sq), (acts_rep, grad_rep))
    return totals


def adamw_update(master, moment_one, moment_two, grad_step, learn_rate):
    mom_one = BETA_ONE * moment_one + (1.0 - BETA_ONE) * grad_step
    mom_two = BETA_TWO * moment_two + (1.0 - BETA_TWO) * grad_step * grad_step
    step_dir = (mom_one / BIAS_ONE) / (jnp.sqrt(mom_two / BIAS_TWO) + ADAM_EPS)
    new_master = master - learn_rate * (step_dir + WEIGHT_DECAY * master)
    return new_master, mom_one, mom_two


def forward_all(weight_up, weight_down, next_micro):
    blocks = next_micro.reshape(MICRO_NEXT * REPLICAS, TOKENS_DEV, D_MODEL)

    def run_block(block):
        def stage_step(stage_in, weights):
            return stage_forward(stage_in, weights[0], weights[1]), None
        result, unused = lax.scan(stage_step, block, (weight_up, weight_down))
        return result
    return lax.map(run_block, blocks).reshape(MICRO_NEXT, REPLICAS * TOKENS_DEV, D_MODEL)


def setup_inputs(seed: int = 0) -> dict:
    keys = jax.random.split(jax.random.key(seed), 16)
    rows = REPLICAS * TOKENS_DEV
    shape_up = (STAGES, D_MODEL, FF_WIDTH)
    shape_down = (STAGES, FF_WIDTH, D_MODEL)
    up_scale = D_MODEL ** -0.5
    down_scale = (FF_WIDTH * STAGES) ** -0.5
    master_up = jax.random.normal(keys[0], shape_up, jnp.float32) * up_scale
    master_down = jax.random.normal(keys[1], shape_down, jnp.float32) * down_scale
    compute_up = master_up.astype(jnp.bfloat16)
    compute_down = master_down.astype(jnp.bfloat16)
    stage_acts = jax.random.normal(keys[2], (STAGES, rows, D_MODEL), jnp.float32).astype(jnp.bfloat16)
    loss_grad = jax.random.normal(keys[3], (rows, D_MODEL), jnp.float32).astype(jnp.bfloat16)
    next_micro = jax.random.normal(keys[4], (MICRO_NEXT, rows, D_MODEL), jnp.float32).astype(jnp.bfloat16)
    sum_up, sum_down, sq_up, sq_down = batch_grads(compute_up, compute_down, stage_acts, loss_grad)
    rms_up = jnp.sqrt(sq_up / (REPLICAS * D_MODEL * FF_WIDTH))
    rms_down = jnp.sqrt(sq_down / (REPLICAS * D_MODEL * FF_WIDTH))
    accum_up = jax.random.normal(keys[5], (REPLICAS,) + shape_up, jnp.float32) * rms_up[None, :, None, None]
    accum_down = jax.random.normal(keys[6], (REPLICAS,) + shape_down, jnp.float32) * rms_down[None, :, None, None]
    avg_up = (jnp.sum(accum_up, axis=0) + sum_up) / REPLICAS
    avg_down = (jnp.sum(accum_down, axis=0) + sum_down) / REPLICAS
    grad_norm = jnp.sqrt(jnp.sum(avg_up * avg_up) + jnp.sum(avg_down * avg_down))
    max_norm = jax.random.uniform(keys[7], (), jnp.float32, 0.35, 0.65) * grad_norm
    clip = jnp.minimum(1.0, max_norm / (grad_norm + NORM_EPS))
    step_up = clip * jnp.sqrt(jnp.mean(avg_up * avg_up, axis=(1, 2)))[:, None, None]
    step_down = clip * jnp.sqrt(jnp.mean(avg_down * avg_down, axis=(1, 2)))[:, None, None]
    moment1_up = jax.random.normal(keys[8], shape_up, jnp.float32) * (0.05 * step_up)
    moment2_up = jax.random.uniform(keys[9], shape_up, jnp.float32, 0.5, 1.5) * (0.025 * step_up * step_up)
    moment1_down = jax.random.normal(keys[10], shape_down, jnp.float32) * (0.05 * step_down)
    moment2_down = jax.random.uniform(keys[11], shape_down, jnp.float32, 0.5, 1.5) * (0.025 * step_down * step_down)
    learn_rate = jax.random.uniform(keys[12], (), jnp.float32, 0.5, 1.0) * (0.1 * up_scale)
    return {'master_up': master_up, 'master_down': master_down,
            'moment1_up': moment1_up, 'moment2_up': moment2_up,
            'moment1_down': moment1_down, 'moment2_down': moment2_down,
            'compute_up': compute_up, 'compute_down': compute_down,
            'accum_up': accum_up, 'accum_down': accum_down,
            'stage_acts': stage_acts, 'loss_grad': loss_grad, 'next_micro': next_micro,
            'learn_rate': learn_rate, 'max_norm': max_norm}


def reference(master_up, master_down, moment1_up, moment2_up, moment1_down, moment2_down,
              compute_up, compute_down, accum_up, accum_down, stage_acts, loss_grad, next_micro,
              learn_rate, max_norm):
    sum_up, sum_down, sq_up, sq_down = batch_grads(compute_up, compute_down, stage_acts, loss_grad)
    avg_up = (jnp.sum(accum_up, axis=0) + sum_up) / REPLICAS
    avg_down = (jnp.sum(accum_down, axis=0) + sum_down) / REPLICAS
    total_sq = jnp.sum(avg_up * avg_up) + jnp.sum(avg_down * avg_down)
    clip = jnp.minimum(1.0, max_norm / (jnp.sqrt(total_sq) + NORM_EPS))
    new_up, mom1_up, mom2_up = adamw_update(master_up, moment1_up, moment2_up, clip * avg_up, learn_rate)
    new_down, mom1_down, mom2_down = adamw_update(master_down, moment1_down, moment2_down, clip * avg_down, learn_rate)
    last_acts = forward_all(new_up.astype(jnp.bfloat16), new_down.astype(jnp.bfloat16), next_micro)
    return (new_up, new_down, mom1_up, mom2_up, mom1_down, mom2_down, last_acts)
```

```python
import functools

import jax
import jax.numpy as jnp
from jax import lax
from jax.experimental import pallas as pl
from jax.experimental.pallas import tpu as pltpu
from jax.sharding import PartitionSpec as P

BETA_ONE = 0.9
BETA_TWO = 0.95
ADAM_EPS = 1e-8
WEIGHT_DECAY = 0.1
NORM_EPS = 1e-6
STEP_NUM = 10
BIAS_ONE = 1.0 - BETA_ONE ** STEP_NUM
BIAS_TWO = 1.0 - BETA_TWO ** STEP_NUM
DOT_ROWS = (((0,), (0,)), ((), ()))
DOT_COLS = (((1,), (1,)), ((), ()))

D_MODEL = 896
FF_WIDTH = 4864
TOKENS = 2048
N_DATA = 4
UP_ROWS = D_MODEL // N_DATA
DOWN_ROWS = FF_WIDTH // N_DATA
GELU_A = 0.7978845608028654
GELU_B = GELU_A * 0.044715
FWD_ROWS = 512
FWD_CHUNKS = (1280, 1280, 1280, 1024)
BACK_CHUNK = 256
VMEM_LIMIT = 63 * 1024 * 1024


def gelu_tanh(u):
    half = 0.5 * u
    return half + half * jnp.tanh(u * (GELU_A + GELU_B * (u * u)))


def gelu_slope(u):
    sq = u * u
    t = jnp.tanh(u * (GELU_A + GELU_B * sq))
    return 0.5 * (1.0 + t) + (0.5 * u) * (1.0 - t * t) * (GELU_A + (3.0 * GELU_B) * sq)


def dot32(a, b, dims=(((1,), (0,)), ((), ()))):
    return lax.dot_general(a, b, dims, preferred_element_type=jnp.float32)


def adamw_update(master, moment_one, moment_two, grad_step, learn_rate):
    mom_one = BETA_ONE * moment_one + (1.0 - BETA_ONE) * grad_step
    mom_two = BETA_TWO * moment_two + (1.0 - BETA_TWO) * grad_step * grad_step
    step_dir = (mom_one / BIAS_ONE) / (jnp.sqrt(mom_two / BIAS_TWO) + ADAM_EPS)
    new_master = master - learn_rate * (step_dir + WEIGHT_DECAY * master)
    return new_master, mom_one, mom_two


def back_one_kernel(acts_ref, grad_ref, up_ref, down_ref, pre_ref, hid_ref, din_ref, total):
    step = pl.program_id(0)

    @pl.when(step == 0)
    def _():
        total[...] = grad_ref[...].astype(jnp.float32)

    for r in range(0, TOKENS, 512):
        rows = pl.ds(r, 512)
        u = dot32(acts_ref[rows, :], up_ref[...])
        pre_ref[rows, :] = u
        hid_ref[rows, :] = gelu_tanh(u).astype(jnp.bfloat16)
        d_hid = dot32(grad_ref[rows, :], down_ref[...], DOT_COLS)
        d_pre = (d_hid * gelu_slope(u)).astype(jnp.bfloat16)
        total[rows, :] += dot32(d_pre, up_ref[...], DOT_COLS)

    @pl.when(step == pl.num_programs(0) - 1)
    def _():
        din_ref[...] = total[...].astype(jnp.bfloat16)


def back_one(acts, grad, w_up, w_down):
    steps = FF_WIDTH // BACK_CHUNK
    whole = pl.BlockSpec((TOKENS, D_MODEL), lambda j: (0, 0))
    cols = pl.BlockSpec((TOKENS, BACK_CHUNK), lambda j: (0, j))
    return pl.pallas_call(
        back_one_kernel,
        grid=(steps,),
        in_specs=[whole, whole, pl.BlockSpec((D_MODEL, BACK_CHUNK), lambda j: (0, j)),
                  pl.BlockSpec((BACK_CHUNK, D_MODEL), lambda j: (j, 0))],
        out_specs=[cols, cols, whole],
        out_shape=[jax.ShapeDtypeStruct((TOKENS, FF_WIDTH), jnp.float32),
                   jax.ShapeDtypeStruct((TOKENS, FF_WIDTH), jnp.bfloat16),
                   jax.ShapeDtypeStruct((TOKENS, D_MODEL), jnp.bfloat16)],
        scratch_shapes=[pltpu.VMEM((TOKENS, D_MODEL), jnp.float32)],
        compiler_params=pltpu.CompilerParams(vmem_limit_bytes=VMEM_LIMIT),
        cost_estimate=pl.CostEstimate(flops=6 * TOKENS * D_MODEL * FF_WIDTH, bytes_accessed=90_000_000, transcendentals=0),
        name='back_one',
    )(acts, grad, w_up, w_down)


def weight_copies(block, up_ref, down_ref, w1, w2, sem):
    found = []
    for d in range(N_DATA):
        found.append(pltpu.make_async_copy(up_ref.at[d, block], w1.at[block, pl.ds(d * UP_ROWS, UP_ROWS)], sem.at[block, d]))
        if down_ref is not None:
            found.append(pltpu.make_async_copy(down_ref.at[d, block], w2.at[block, pl.ds(d * DOWN_ROWS, DOWN_ROWS)], sem.at[block, N_DATA + d]))
    return found


def hidden_kernel(stage_ref, x_ref, up_ref, hid_ref, w1, sem):
    @pl.when(pl.program_id(0) == 0)
    def _():
        copies = weight_copies(0, up_ref, None, w1, None, sem)
        for c in copies:
            c.start()
        for c in copies:
            c.wait()

    off = 0
    for width in FWD_CHUNKS:
        u = dot32(x_ref[0], w1[0, :, off:off + width])
        hid_ref[0, :, off:off + width] = gelu_tanh(u).astype(jnp.bfloat16)
        off += width


def forward_kernel(has_hidden, *refs):
    refs = list(refs)
    _, x_ref = refs[:2]
    hid_ref = refs[2] if has_hidden else None
    up_ref, down_ref, out_ref, send_ref, w1, w2, sem = refs[-7:]
    step = pl.program_id(0)

    @pl.when(step == 0)
    def _():
        for block in range(2):
            for c in weight_copies(block, up_ref, down_ref, w1, w2, sem):
                c.start()

    x = x_ref[0]
    for block in range(2):
        @pl.when(step == 0)
        def _():
            for c in weight_copies(block, up_ref, down_ref, w1, w2, sem):
                c.wait()

        total = x.astype(jnp.float32)
        off = 0
        for width in FWD_CHUNKS:
            if block == 0 and has_hidden:
                h = hid_ref[0, :, off:off + width]
            else:
                h = gelu_tanh(dot32(x, w1[block, :, off:off + width])).astype(jnp.bfloat16)
            total = total + dot32(h, w2[block, off:off + width, :])
            off += width
        x = total.astype(jnp.bfloat16)
    send_ref[0] = x
    out_ref[0] = x


def own_spec(micro_per, start):
    row_blocks = TOKENS // FWD_ROWS
    return pl.BlockSpec((1, FWD_ROWS, D_MODEL),
                        lambda i, st: (st[0] * micro_per + start + i // row_blocks, i % row_blocks, 0))


def hidden_call(stage, micro, full_up, start, count):
    row_blocks = TOKENS // FWD_ROWS
    return pl.pallas_call(
        hidden_kernel,
        grid_spec=pltpu.PrefetchScalarGridSpec(
            num_scalar_prefetch=1, grid=(count * row_blocks,),
            in_specs=[own_spec(micro.shape[0] // 2, start), pl.BlockSpec(memory_space=pl.ANY)],
            out_specs=pl.BlockSpec((1, FWD_ROWS, FF_WIDTH), lambda i, st: (i // row_blocks, i % row_blocks, 0)),
            scratch_shapes=[pltpu.VMEM((1, D_MODEL, FF_WIDTH), jnp.bfloat16), pltpu.SemaphoreType.DMA((1, N_DATA))]),
        out_shape=jax.ShapeDtypeStruct((count, TOKENS, FF_WIDTH), jnp.bfloat16),
        compiler_params=pltpu.CompilerParams(vmem_limit_bytes=VMEM_LIMIT),
        cost_estimate=pl.CostEstimate(flops=2 * count * TOKENS * D_MODEL * FF_WIDTH, bytes_accessed=count * 24_000_000, transcendentals=0),
        name='hidden_call',
    )(stage, micro, full_up)


def forward_call(stage, micro, full_up, full_down, start, count, hidden=None, into=None):
    row_blocks = TOKENS // FWD_ROWS
    spec = own_spec(micro.shape[0] // 2, start)
    any_spec = pl.BlockSpec(memory_space=pl.ANY)
    args, in_specs = [stage, micro], [spec]
    if hidden is not None:
        args.append(hidden)
        in_specs.append(pl.BlockSpec((1, FWD_ROWS, FF_WIDTH), lambda i, st: (i // row_blocks, i % row_blocks, 0)))
    aliases = {}
    if into is not None:
        aliases = {len(args): 0}
        args.append(into)
        in_specs.append(any_spec)
    args += [full_up, full_down]
    in_specs += [any_spec, any_spec]
    return pl.pallas_call(
        functools.partial(forward_kernel, hidden is not None),
        grid_spec=pltpu.PrefetchScalarGridSpec(
            num_scalar_prefetch=1, grid=(count * row_blocks,),
            in_specs=in_specs,
            out_specs=[spec, pl.BlockSpec((1, FWD_ROWS, D_MODEL), lambda i, st: (i // row_blocks, i % row_blocks, 0))],
            scratch_shapes=[pltpu.VMEM((2, D_MODEL, FF_WIDTH), jnp.bfloat16), pltpu.VMEM((2, FF_WIDTH, D_MODEL), jnp.bfloat16),
                            pltpu.SemaphoreType.DMA((2, 2 * N_DATA))]),
        out_shape=[jax.ShapeDtypeStruct(micro.shape, jnp.bfloat16),
                   jax.ShapeDtypeStruct((count, TOKENS, D_MODEL), jnp.bfloat16)],
        input_output_aliases=aliases,
        compiler_params=pltpu.CompilerParams(vmem_limit_bytes=VMEM_LIMIT),
        cost_estimate=pl.CostEstimate(flops=8 * count * TOKENS * D_MODEL * FF_WIDTH, bytes_accessed=count * 30_000_000, transcendentals=0),
        name='forward_call',
    )(*args)


def solution(mesh):
    n_data = mesh.shape['data']

    def step_body(master_up, master_down, moment1_up, moment2_up, moment1_down, moment2_down,
                  compute_up, compute_down, accum_up, accum_down, stage_acts, loss_grad, next_micro,
                  learn_rate, max_norm):
        my_stage = lax.axis_index('stage')
        stage = my_stage.astype(jnp.int32)[None]
        acts, w_up, w_down = stage_acts[0], compute_up[0], compute_down[0]

        pre_act, hidden, d_in = back_one(acts, loss_grad, w_up, w_down)
        below = lax.ppermute(d_in, 'stage', [(1, 0)])
        grad_in = jnp.where(my_stage == 1, loss_grad, below)
        sum_down = accum_down[0, 0] + dot32(hidden, grad_in, DOT_ROWS)
        sum_down, grad_in = lax.optimization_barrier((sum_down, grad_in))
        shard_down = lax.psum_scatter(sum_down, 'data', scatter_dimension=0, tiled=True) / n_data
        d_hid = dot32(grad_in, w_down, DOT_COLS)
        d_pre = (d_hid * gelu_slope(pre_act)).astype(jnp.bfloat16)
        sum_up = accum_up[0, 0] + dot32(acts, d_pre, DOT_ROWS)
        shard_up = lax.psum_scatter(sum_up, 'data', scatter_dimension=0, tiled=True) / n_data

        local_sq = jnp.sum(shard_up * shard_up) + jnp.sum(shard_down * shard_down)
        total_sq = lax.psum(local_sq, ('stage', 'data'))
        clip = jnp.minimum(1.0, max_norm / (jnp.sqrt(total_sq) + NORM_EPS))
        new_up, mom1_up, mom2_up = adamw_update(master_up[0], moment1_up[0], moment2_up[0], clip * shard_up, learn_rate)
        full_up = lax.all_gather(new_up.astype(jnp.bfloat16), ('data', 'stage'))
        full_up = full_up.reshape(N_DATA, 2, UP_ROWS, FF_WIDTH)
        new_down, mom1_down, mom2_down = adamw_update(master_down[0], moment1_down[0], moment2_down[0], clip * shard_down, learn_rate)
        full_down = lax.all_gather(new_down.astype(jnp.bfloat16), ('data', 'stage'))
        full_down = full_down.reshape(N_DATA, 2, DOWN_ROWS, D_MODEL)

        half = next_micro.shape[0] // 2
        swap = [(0, 1), (1, 0)]
        hid = hidden_call(stage, next_micro, full_up, 0, 4)
        out, sent_a = forward_call(stage, next_micro, full_up, full_down, 0, 4, hidden=hid)
        got_a = lax.ppermute(sent_a, 'stage', swap)
        out, sent_b = forward_call(stage, next_micro, full_up, full_down, 4, 3, into=out)
        got_b = lax.ppermute(sent_b, 'stage', swap)
        out, sent_c = forward_call(stage, next_micro, full_up, full_down, 7, 1, into=out)
        got_c = lax.ppermute(sent_c, 'stage', swap)
        other = (1 - my_stage) * half
        out = lax.dynamic_update_slice(out, got_a, (other, 0, 0))
        out = lax.dynamic_update_slice(out, got_b, (other + 4, 0, 0))
        last_acts = lax.dynamic_update_slice(out, got_c, (other + 7, 0, 0))
        return (new_up[None], new_down[None], mom1_up[None], mom2_up[None],
                mom1_down[None], mom2_down[None], last_acts)

    shard_spec = P('stage', 'data', None)
    whole_spec = P('stage', None, None)
    accum_spec = P('data', 'stage', None, None)
    micro_spec = P(None, 'data', None)
    in_specs = (shard_spec,) * 6 + (whole_spec, whole_spec, accum_spec, accum_spec,
                                    P('stage', 'data', None), P('data', None), micro_spec, P(), P())
    out_specs = (shard_spec,) * 6 + (micro_spec,)
    return jax.shard_map(step_body, mesh=mesh, in_specs=in_specs, out_specs=out_specs, check_vma=False)
```
